32 devices in a mesh: zero: 16 (over z, y, core), width: 2 (over x).
Axes of the slice: x: 2, y: 2, z: 4, core: 2. Of those that a mesh axis runs over, the one named last changes fastest.
Arguments:
- slopes_in: float32 [128, 128, 4096], P(None, 'zero', 'width'), may hold values from -6 to 6
- moments_in: float32 [128, 128, 4096], P(None, 'zero', 'width'), may hold values from -6 to 6
- weights_in: float32 [128, 128, 4096], P(None, 'zero', 'width'), may hold values from -0.1875 to 0.1875
Outputs:
- new_weights: float32 [128, 128, 4096], P(None, 'zero', 'width')
- new_momentum: float32 [128, 128, 4096], P(None, 'zero', 'width')
The draws below stay inside these ranges and needn't reach their ends.
All inputs are finite; a program needn't handle non-finite values.
Results may differ from the reference program's by a relative error of at most 0.0001.
Values sent between devices are 32-bit elements; how exact they have to be, the bound alone decides.
A program may use at most 128 MiB of HBM per device.

```python
import jax
import jax.numpy as jnp
from jax import lax

SIDE = 128
WIDE = 4096
MATS = 128
ITERS = 3


def level_of(stream_key, shape, pieces, smallest, high):
    def one(dim, parts):
        draws = jax.random.uniform(jax.random.fold_in(jax.random.fold_in(stream_key, 6), dim), (parts,), jnp.float32, smallest / len(pieces), high / len(pieces))
        return jnp.repeat(jnp.exp(draws), shape[dim] // parts).reshape((-1,) + (1,) * (len(shape) - dim - 1))

    factor_of = one(*pieces[0])
    for cut in pieces[1:]:
        factor_of = factor_of * one(*cut)
    return factor_of


def normal_values(rng, extent, spread, limit, cuts=(), held_as=jnp.bfloat16):
    values = jax.random.normal(rng, extent, jnp.float32) * spread
    if len(cuts) > 0:
        values = level_of(rng, extent, cuts, -0.22, 0.18) * values
    return jnp.clip(values, min=-limit, max=limit).astype(held_as)


def setup_inputs(seed: int = 0) -> dict:
    keys = jax.random.split(jax.random.key(seed), 4)
    slopes_in = normal_values(keys[0], (MATS, SIDE, WIDE), 1.0, 6.0, ((1, 16), (2, 2)), jnp.float32)
    moments_in = normal_values(keys[1], (MATS, SIDE, WIDE), 1.0, 6.0, ((1, 16), (2, 2)), jnp.float32)
    weights_in = normal_values(keys[2], (MATS, SIDE, WIDE), 0.03, 0.1875, ((1, 16), (2, 2)), jnp.float32)
    return dict(slopes_in=slopes_in, moments_in=moments_in, weights_in=weights_in)


hold_rate = 0.8
learn_rate = 0.8
decay_rate = 0.1

def reference(slopes_in, moments_in, weights_in):
    new_momentum = hold_rate * moments_in + slopes_in
    direction = hold_rate * new_momentum + slopes_in

    def orthogonal_one(stack):
        iterate = stack[None]
        iterate = iterate * lax.rsqrt(lax.optimization_barrier(jnp.sum(iterate * iterate, axis=(1, 2), keepdims=True)) + 1e-06)
        for step in range(ITERS):
            gram = jnp.einsum('mik,mjk->mij', iterate, iterate, precision=lax.Precision.HIGHEST)
            mixed = -4.775 * gram + 2.0315 * jnp.einsum('mij,mjk->mik', gram, gram, precision=lax.Precision.HIGHEST)
            iterate = 3.4445 * iterate + jnp.einsum('mij,mjk->mik', mixed, iterate, precision=lax.Precision.HIGHEST)
        return iterate[0]
    iterate = lax.map(orthogonal_one, direction)
    new_weights = (1.0 - learn_rate * decay_rate) * weights_in - learn_rate * iterate
    return (new_weights, new_momentum)
```

```python
import functools

import jax
import jax.numpy as jnp
from jax import lax
from jax.experimental import pallas as pl
from jax.experimental.pallas import tpu as pltpu
from jax.sharding import PartitionSpec as P

ITERS = 3
MESH = pl.DeviceIdType.MESH

hold_rate = 0.8
learn_rate = 0.8
decay_rate = 0.1


def dot(a, b):
    return jnp.dot(a, b, precision=lax.Precision.HIGHEST, preferred_element_type=jnp.float32)


def kernel(
    nz, nw, slopes, moments, weights, res, mom, sent, held, made, back, gram, heard,
    slope_sem, moment_sem, weight_sem, fwd_send, fwd_recv, own_sem, gram_send, gram_recv, ret_send, ret_recv,
):
    me = lax.axis_index("zero")
    side = lax.axis_index("width")
    _, mine, rows, cols = sent.shape
    total_rows = nz * rows
    half = nz // 2
    my_half = me // half

    def far(k):
        return (1 - my_half) * half + lax.rem(me + k, half)

    def near(k):
        return my_half * half + lax.rem(me + k, half)

    barrier = pltpu.get_barrier_semaphore()

    def greet_zero(k, c):
        pl.semaphore_signal(barrier, inc=1, device_id=(lax.rem(me + k, nz), side), device_id_type=MESH)
        return c

    def greet_width(k, c):
        pl.semaphore_signal(barrier, inc=1, device_id=(me, lax.rem(side + k, nw)), device_id_type=MESH)
        return c

    lax.fori_loop(1, nz, greet_zero, 0)
    lax.fori_loop(1, nw, greet_width, 0)

    def load(j, c):
        pltpu.make_async_copy(slopes.at[:, j], sent.at[:, j], slope_sem.at[j]).start()
        pltpu.make_async_copy(moments.at[:, j], mom.at[:, j], moment_sem.at[j]).start()
        return c

    lax.fori_loop(0, mine, load, 0)

    def direction(j):
        pltpu.make_async_copy(slopes.at[:, j], sent.at[:, j], slope_sem.at[j]).wait()
        pltpu.make_async_copy(moments.at[:, j], mom.at[:, j], moment_sem.at[j]).wait()

        def one(k, c):
            slope = sent[k, j]
            fresh = hold_rate * mom[k, j] + slope
            mom[k, j] = fresh
            sent[k, j] = hold_rate * fresh + slope
            return c

        lax.fori_loop(0, nz, one, 0)

    def send(j, to):
        pltpu.make_async_remote_copy(
            src_ref=sent.at[to, j],
            dst_ref=held.at[j, me],
            send_sem=fwd_send,
            recv_sem=fwd_recv.at[j],
            device_id=(to, side),
            device_id_type=MESH,
        ).start()

    def forward(j):
        def far_one(k, c):
            send(j, far(k))
            return c

        def near_one(k, c):
            send(j, near(k))
            return c

        lax.fori_loop(0, half, far_one, 0)
        lax.fori_loop(1, half, near_one, 0)
        pltpu.make_async_copy(sent.at[me, j], held.at[j, me], own_sem.at[j]).start()

    direction(0)
    pl.semaphore_wait(barrier, nz - 1 + nw - 1)

    def ahead(j, c):
        forward(j - 1)
        direction(j)
        return c

    lax.fori_loop(1, mine, ahead, 0)
    forward(mine - 1)
    pltpu.make_async_copy(weights, res, weight_sem).start()

    def gram_of(j):
        others = held.at[j, pl.ds(0, nz - 1)]
        pltpu.make_async_copy(others, others, fwd_recv.at[j]).wait()
        pltpu.make_async_copy(sent.at[me, j], held.at[j, me], own_sem.at[j]).wait()
        x = held[j].reshape(total_rows, cols)
        gram[j] = lax.dot_general(
            x, x, (((1,), (1,)), ((), ())),
            precision=lax.Precision.HIGHEST, preferred_element_type=jnp.float32,
        )

        def one(k, c):
            to = lax.rem(side + k, nw)
            pltpu.make_async_remote_copy(
                src_ref=gram.at[j],
                dst_ref=heard.at[j, k - 1],
                send_sem=gram_send,
                recv_sem=gram_recv.at[j],
                device_id=(me, to),
                device_id_type=MESH,
            ).start()
            return c

        lax.fori_loop(1, nw, one, 0)

    def give(j, to):
        pltpu.make_async_remote_copy(
            src_ref=made.at[j, to],
            dst_ref=back.at[me, j],
            send_sem=ret_send,
            recv_sem=ret_recv.at[j],
            device_id=(to, side),
            device_id_type=MESH,
        ).start()

    def finish(j):
        pltpu.make_async_copy(heard.at[j], heard.at[j], gram_recv.at[j]).wait()
        full = gram[j] + jnp.sum(heard[j], axis=0)
        at_diag = lax.broadcasted_iota(jnp.int32, full.shape, 0) == lax.broadcasted_iota(jnp.int32, full.shape, 1)
        squares = jnp.sum(jnp.sum(jnp.where(at_diag, full, 0.0), axis=1, keepdims=True), axis=0, keepdims=True)
        scale = lax.rsqrt(squares + 1e-06)
        a = full * scale * scale
        eye = jnp.where(at_diag, 3.4445, 0.0)
        mix = None
        for step in range(ITERS):
            m = eye - 4.775 * a + 2.0315 * dot(a, a)
            if step < ITERS - 1:
                a = dot(dot(m, a), m)
            mix = m if mix is None else dot(m, mix)
        mix = mix * scale
        y = dot(mix, held[j].reshape(total_rows, cols))
        made[j] = y.reshape(nz, rows, cols)

        def far_one(k, c):
            give(j, far(k))
            return c

        def near_one(k, c):
            give(j, near(k))
            return c

        lax.fori_loop(0, half, far_one, 0)
        lax.fori_loop(1, half, near_one, 0)
        back[me, j] = made[j, me]

    gram_of(0)

    def stage(j, c):
        gram_of(j)
        finish(j - 1)
        return c

    lax.fori_loop(1, mine, stage, 0)
    finish(mine - 1)

    pltpu.make_async_copy(weights, res, weight_sem).wait()

    def update(j, c):
        came = back.at[pl.ds(0, nz - 1), j]
        pltpu.make_async_copy(came, came, ret_recv.at[j]).wait()

        def one(k, c):
            res[k, j] = (1.0 - learn_rate * decay_rate) * res[k, j] - learn_rate * back[k, j]
            return c

        return lax.fori_loop(0, nz, one, c)

    lax.fori_loop(0, mine, update, 0)

    others = sent.at[pl.ds(0, nz - 1)]
    pltpu.make_async_copy(others, others, fwd_send).wait()
    pltpu.make_async_copy(heard, heard, gram_send).wait()
    pltpu.make_async_copy(others, others, ret_send).wait()


def stepped(nz, nw, slopes, moments, weights):
    mats, rows, cols = slopes.shape
    mine = mats // nz
    n = nz * rows
    split = (nz, mine, rows, cols)
    hbm = pl.BlockSpec(memory_space=pltpu.HBM)
    buffer = pltpu.VMEM(split, jnp.float32)
    gathered = pltpu.VMEM((mine, nz, rows, cols), jnp.float32)
    each = pltpu.SemaphoreType.DMA((mine,))
    once = pltpu.SemaphoreType.DMA
    out, mom = pl.pallas_call(
        functools.partial(kernel, nz, nw),
        out_shape=(pltpu.VMEM(split, jnp.float32),) * 2,
        in_specs=[hbm] * 3,
        out_specs=[pl.BlockSpec(memory_space=pltpu.VMEM)] * 2,
        scratch_shapes=[
            buffer,
            gathered,
            gathered,
            buffer,
            pltpu.VMEM((mine, n, n), jnp.float32),
            pltpu.VMEM((mine, nw - 1, n, n), jnp.float32),
            each,
            each,
            once,
            once,
            each,
            each,
            once,
            each,
            once,
            each,
        ],
        compiler_params=pltpu.CompilerParams(
            collective_id=0, has_side_effects=True, vmem_limit_bytes=35 * 1024 * 1024
        ),
        name="stepped",
    )(slopes.reshape(split), moments.reshape(split), weights.reshape(split))
    return out.reshape(slopes.shape), mom.reshape(slopes.shape)


def body(nz, nw, slopes_in, moments_in, weights_in):
    return stepped(nz, nw, slopes_in, moments_in, weights_in)


def solution(mesh):
    spec = P(None, "zero", "width")
    run = functools.partial(body, mesh.shape["zero"], mesh.shape["width"])
    return jax.shard_map(run, mesh=mesh, in_specs=(spec,) * 3, out_specs=(spec,) * 2, check_vma=False)
```

```python
import functools

import jax
import jax.numpy as jnp
from jax import lax
from jax.experimental import pallas as pl
from jax.experimental.pallas import tpu as pltpu
from jax.sharding import PartitionSpec as P

ITERS = 3
MESH = pl.DeviceIdType.MESH

hold_rate = 0.8
learn_rate = 0.8
decay_rate = 0.1


def dot(a, b):
    return jnp.dot(a, b, precision=lax.Precision.HIGHEST, preferred_element_type=jnp.float32)


def kernel(
    nz, nw, slopes, moments, weights, res, mom, sent, held, made, back, gram, heard,
    slope_sem, moment_sem, weight_sem, fwd_send, fwd_recv, own_sem, gram_send, gram_recv, ret_send, ret_recv,
):
    me = lax.axis_index("zero")
    side = lax.axis_index("width")
    _, mine, rows, cols = sent.shape
    total_rows = nz * rows
    half = nz // 2
    quarter = nz // 4
    my_half = me // half

    def far(k):
        outer = 1 - k // quarter
        return (1 - my_half) * (half + outer * quarter) + my_half * (1 - outer) * quarter + lax.rem(me + k, quarter)

    def near(k):
        return my_half * half + lax.rem(me + k, half)

    barrier = pltpu.get_barrier_semaphore()

    def greet_zero(k, c):
        pl.semaphore_signal(barrier, inc=1, device_id=(lax.rem(me + k, nz), side), device_id_type=MESH)
        return c

    def greet_width(k, c):
        pl.semaphore_signal(barrier, inc=1, device_id=(me, lax.rem(side + k, nw)), device_id_type=MESH)
        return c

    lax.fori_loop(1, nz, greet_zero, 0)
    lax.fori_loop(1, nw, greet_width, 0)

    def load(j, c):
        pltpu.make_async_copy(slopes.at[:, j], sent.at[:, j], slope_sem.at[j]).start()
        pltpu.make_async_copy(moments.at[:, j], mom.at[:, j], moment_sem.at[j]).start()
        return c

    load(0, 0)

    def direction(j):
        pltpu.make_async_copy(slopes.at[:, j], sent.at[:, j], slope_sem.at[j]).wait()
        pltpu.make_async_copy(moments.at[:, j], mom.at[:, j], moment_sem.at[j]).wait()

        def one(k, c):
            slope = sent[k, j]
            fresh = hold_rate * mom[k, j] + slope
            mom[k, j] = fresh
            sent[k, j] = hold_rate * fresh + slope
            return c

        lax.fori_loop(0, nz, one, 0)

    def send(j, to):
        pltpu.make_async_remote_copy(
            src_ref=sent.at[to, j],
            dst_ref=held.at[j, me],
            send_sem=fwd_send,
            recv_sem=fwd_recv.at[j],
            device_id=(to, side),
            device_id_type=MESH,
        ).start()

    def forward(j):
        def far_one(k, c):
            send(j, far(k))
            return c

        def near_one(k, c):
            send(j, near(k))
            return c

        lax.fori_loop(0, half, far_one, 0)
        lax.fori_loop(1, half, near_one, 0)
        pltpu.make_async_copy(sent.at[me, j], held.at[j, me], own_sem.at[j]).start()

    direction(0)
    lax.fori_loop(1, mine, load, 0)
    pl.semaphore_wait(barrier, nz - 1 + nw - 1)

    def ahead(j, c):
        forward(j - 1)
        direction(j)
        return c

    lax.fori_loop(1, mine, ahead, 0)
    forward(mine - 1)
    pltpu.make_async_copy(weights, res, weight_sem).start()

    def gram_of(j):
        others = held.at[j, pl.ds(0, nz - 1)]
        pltpu.make_async_copy(others, others, fwd_recv.at[j]).wait()
        pltpu.make_async_copy(sent.at[me, j], held.at[j, me], own_sem.at[j]).wait()
        x = held[j].reshape(total_rows, cols)
        gram[j] = lax.dot_general(
            x, x, (((1,), (1,)), ((), ())),
            precision=lax.Precision.HIGHEST, preferred_element_type=jnp.float32,
        )

        def one(k, c):
            to = lax.rem(side + k, nw)
            pltpu.make_async_remote_copy(
                src_ref=gram.at[j],
                dst_ref=heard.at[j, k - 1],
                send_sem=gram_send,
                recv_sem=gram_recv.at[j],
                device_id=(me, to),
                device_id_type=MESH,
            ).start()
            return c

        lax.fori_loop(1, nw, one, 0)

    def give(j, to):
        pltpu.make_async_remote_copy(
            src_ref=made.at[j, to],
            dst_ref=back.at[me, j],
            send_sem=ret_send,
            recv_sem=ret_recv.at[j],
            device_id=(to, side),
            device_id_type=MESH,
        ).start()

    def finish(j):
        pltpu.make_async_copy(heard.at[j], heard.at[j], gram_recv.at[j]).wait()
        full = gram[j] + jnp.sum(heard[j], axis=0)
        at_diag = lax.broadcasted_iota(jnp.int32, full.shape, 0) == lax.broadcasted_iota(jnp.int32, full.shape, 1)
        squares = jnp.sum(jnp.sum(jnp.where(at_diag, full, 0.0), axis=1, keepdims=True), axis=0, keepdims=True)
        scale = lax.rsqrt(squares + 1e-06)
        a = full * scale * scale
        eye = jnp.where(at_diag, 3.4445, 0.0)
        mix = None
        for step in range(ITERS):
            m = eye - 4.775 * a + 2.0315 * dot(a, a)
            if step < ITERS - 1:
                a = dot(dot(m, a), m)
            mix = m if mix is None else dot(m, mix)
        mix = mix * scale
        y = dot(mix, held[j].reshape(total_rows, cols))
        made[j] = y.reshape(nz, rows, cols)

        def far_one(k, c):
            give(j, far(k))
            return c

        def near_one(k, c):
            give(j, near(k))
            return c

        lax.fori_loop(0, half, far_one, 0)
        lax.fori_loop(1, half, near_one, 0)
        back[me, j] = made[j, me]

    gram_of(0)

    def stage(j, c):
        gram_of(j)
        finish(j - 1)
        return c

    lax.fori_loop(1, mine, stage, 0)
    finish(mine - 1)

    pltpu.make_async_copy(weights, res, weight_sem).wait()

    def update(j, c):
        came = back.at[pl.ds(0, nz - 1), j]
        pltpu.make_async_copy(came, came, ret_recv.at[j]).wait()

        def one(k, c):
            res[k, j] = (1.0 - learn_rate * decay_rate) * res[k, j] - learn_rate * back[k, j]
            return c

        return lax.fori_loop(0, nz, one, c)

    lax.fori_loop(0, mine, update, 0)

    others = sent.at[pl.ds(0, nz - 1)]
    pltpu.make_async_copy(others, others, fwd_send).wait()
    pltpu.make_async_copy(heard, heard, gram_send).wait()
    pltpu.make_async_copy(others, others, ret_send).wait()


def leave(res, mom, new_weights, new_momentum, sems):
    def copies(k):
        return (
            pltpu.make_async_copy(res.at[k], new_weights.at[k], sems.at[0, k]),
            pltpu.make_async_copy(mom.at[k], new_momentum.at[k], sems.at[1, k]),
        )

    def go(k, c):
        for copy in copies(k):
            copy.start()
        return c

    def end(k, c):
        for copy in copies(k):
            copy.wait()
        return c

    lax.fori_loop(0, res.shape[0], go, 0)
    lax.fori_loop(0, res.shape[0], end, 0)


def stepped(nz, nw, slopes, moments, weights):
    mats, rows, cols = slopes.shape
    mine = mats // nz
    n = nz * rows
    split = (nz, mine, rows, cols)
    hbm = pl.BlockSpec(memory_space=pltpu.HBM)
    buffer = pltpu.VMEM(split, jnp.float32)
    gathered = pltpu.VMEM((mine, nz, rows, cols), jnp.float32)
    each = pltpu.SemaphoreType.DMA((mine,))
    once = pltpu.SemaphoreType.DMA
    out, mom = pl.pallas_call(
        functools.partial(kernel, nz, nw),
        out_shape=(pltpu.VMEM(split, jnp.float32),) * 2,
        in_specs=[hbm] * 3,
        out_specs=[pl.BlockSpec(memory_space=pltpu.VMEM)] * 2,
        scratch_shapes=[
            buffer,
            gathered,
            gathered,
            buffer,
            pltpu.VMEM((mine, n, n), jnp.float32),
            pltpu.VMEM((mine, nw - 1, n, n), jnp.float32),
            each,
            each,
            once,
            once,
            each,
            each,
            once,
            each,
            once,
            each,
        ],
        compiler_params=pltpu.CompilerParams(
            collective_id=0, has_side_effects=True, vmem_limit_bytes=35 * 1024 * 1024
        ),
        name="stepped",
    )(slopes.reshape(split), moments.reshape(split), weights.reshape(split))
    out, mom = pl.pallas_call(
        leave,
        out_shape=(jax.ShapeDtypeStruct(split, jnp.float32),) * 2,
        in_specs=[pl.BlockSpec(memory_space=pltpu.VMEM)] * 2,
        out_specs=[hbm] * 2,
        scratch_shapes=[pltpu.SemaphoreType.DMA((2, nz))],
        compiler_params=pltpu.CompilerParams(vmem_limit_bytes=1024 * 1024),
        name="leave",
    )(out, mom)
    return out.reshape(slopes.shape), mom.reshape(slopes.shape)


def body(nz, nw, slopes_in, moments_in, weights_in):
    return stepped(nz, nw, slopes_in, moments_in, weights_in)


def solution(mesh):
    spec = P(None, "zero", "width")
    run = functools.partial(body, mesh.shape["zero"], mesh.shape["width"])
    return jax.shard_map(run, mesh=mesh, in_specs=(spec,) * 3, out_specs=(spec,) * 2, check_vma=False)
```

```python
import functools

import jax
import jax.numpy as jnp
from jax import lax
from jax.experimental import pallas as pl
from jax.experimental.pallas import tpu as pltpu
from jax.sharding import PartitionSpec as P

ITERS = 3
MESH = pl.DeviceIdType.MESH

hold_rate = 0.8
learn_rate = 0.8
decay_rate = 0.1


def dot(a, b):
    return jnp.dot(a, b, precision=lax.Precision.HIGHEST, preferred_element_type=jnp.float32)


def kernel(
    nz, nw, slopes, moments, weights, res, mom, sent, held, made, back, gram, heard,
    slope_sem, moment_sem, weight_sem, fwd_send, fwd_recv, own_sem, gram_send, gram_recv, ret_send, ret_recv,
):
    me = lax.axis_index("zero")
    side = lax.axis_index("width")
    _, mine, rows, cols = sent.shape
    total_rows = nz * rows
    half = nz // 2
    quarter = nz // 4
    my_half = me // half
    my_quarter = me // quarter
    inner = jnp.logical_and(my_quarter >= 1, my_quarter <= 2)
    partner = my_half * quarter + (1 - my_half) * half + lax.rem(me, quarter)

    def far(k):
        outer = 1 - k // quarter
        return (1 - my_half) * (half + outer * quarter) + my_half * (1 - outer) * quarter + lax.rem(me + k, quarter)

    def near(k):
        return my_half * half + lax.rem(me + k, half)

    barrier = pltpu.get_barrier_semaphore()

    def greet(to, across):
        pl.semaphore_signal(barrier, inc=1, device_id=(to, lax.rem(side + across, nw)), device_id_type=MESH)

    def inner_of(k):
        return quarter + lax.rem(me + quarter + k, half)

    def outer_of(k):
        return lax.rem(half + quarter + lax.rem(me + quarter + k, half), nz)

    @pl.when(inner)
    def _():
        greet(partner, 0)

    @pl.when(jnp.logical_not(inner))
    def _():
        def greet_outer(k, c):
            greet(outer_of(k), 0)
            return c

        def greet_across(k, c):
            greet(me, k)
            return c

        lax.fori_loop(1, half, greet_outer, 0)
        lax.fori_loop(1, nw, greet_across, 0)

    def slope_copy(k):
        return pltpu.make_async_copy(slopes.at[k], sent.at[k], slope_sem.at[k])

    def moment_copy(k):
        return pltpu.make_async_copy(moments.at[k], mom.at[k], moment_sem.at[k])

    def load(k):
        slope_copy(k).start()
        moment_copy(k).start()

    def direction(k):
        slope_copy(k).wait()
        moment_copy(k).wait()

        def one(j, c):
            slope = sent[k, j]
            fresh = hold_rate * mom[k, j] + slope
            mom[k, j] = fresh
            sent[k, j] = hold_rate * fresh + slope
            return c

        lax.fori_loop(0, mine, one, 0)

    def send(j, to):
        pltpu.make_async_remote_copy(
            src_ref=sent.at[to, j],
            dst_ref=held.at[j, me],
            send_sem=fwd_send,
            recv_sem=fwd_recv.at[j],
            device_id=(to, side),
            device_id_type=MESH,
        ).start()

    def other(k):
        return lax.rem(partner + k, nz)

    load(partner)

    def load_one(k, c):
        load(other(k))
        return c

    def direction_one(k, c):
        direction(other(k))
        return c

    direction(partner)
    lax.fori_loop(1, nz, load_one, 0)

    @pl.when(inner)
    def _():
        pl.semaphore_wait(barrier, 1)

        def early(j, c):
            send(j, partner)
            return c

        lax.fori_loop(0, mine, early, 0)

        def greet_outer(k, c):
            def one(across, c):
                greet(outer_of(k), across)
                return c

            return lax.fori_loop(0, nw, one, c)

        lax.fori_loop(0, half, greet_outer, 0)

    lax.fori_loop(1, nz, direction_one, 0)

    @pl.when(inner)
    def _():
        pl.semaphore_wait(barrier, half)

    @pl.when(jnp.logical_not(inner))
    def _():
        pl.semaphore_wait(barrier, half - 1 + nw - 1 + half * nw)

        def greet_inner(k, c):
            greet(inner_of(k), 0)
            return c

        lax.fori_loop(0, half, greet_inner, 0)

    def forward(j, c):
        def far_one(k, c):
            send(j, far(k))
            return c

        def near_one(k, c):
            send(j, near(k))
            return c

        lax.fori_loop(0, quarter, far_one, 0)

        @pl.when(inner)
        def _():
            lax.fori_loop(quarter + 1, half, far_one, 0)

        @pl.when(jnp.logical_not(inner))
        def _():
            lax.fori_loop(quarter, half, far_one, 0)

        lax.fori_loop(1, half, near_one, 0)
        pltpu.make_async_copy(sent.at[me, j], held.at[j, me], own_sem.at[j]).start()
        return c

    lax.fori_loop(0, mine, forward, 0)
    pltpu.make_async_copy(weights, res, weight_sem).start()

    def gram_of(j):
        others = held.at[j, pl.ds(0, nz - 1)]
        pltpu.make_async_copy(others, others, fwd_recv.at[j]).wait()
        pltpu.make_async_copy(sent.at[me, j], held.at[j, me], own_sem.at[j]).wait()
        x = held[j].reshape(total_rows, cols)
        gram[j] = lax.dot_general(
            x, x, (((1,), (1,)), ((), ())),
            precision=lax.Precision.HIGHEST, preferred_element_type=jnp.float32,
        )

        def one(k, c):
            to = lax.rem(side + k, nw)
            pltpu.make_async_remote_copy(
                src_ref=gram.at[j],
                dst_ref=heard.at[j, k - 1],
                send_sem=gram_send,
                recv_sem=gram_recv.at[j],
                device_id=(me, to),
                device_id_type=MESH,
            ).start()
            return c

        lax.fori_loop(1, nw, one, 0)

    def give(j, to):
        pltpu.make_async_remote_copy(
            src_ref=made.at[j, to],
            dst_ref=back.at[me, j],
            send_sem=ret_send,
            recv_sem=ret_recv.at[j],
            device_id=(to, side),
            device_id_type=MESH,
        ).start()

    def finish(j):
        pltpu.make_async_copy(heard.at[j], heard.at[j], gram_recv.at[j]).wait()
        full = gram[j] + jnp.sum(heard[j], axis=0)
        at_diag = lax.broadcasted_iota(jnp.int32, full.shape, 0) == lax.broadcasted_iota(jnp.int32, full.shape, 1)
        squares = jnp.sum(jnp.sum(jnp.where(at_diag, full, 0.0), axis=1, keepdims=True), axis=0, keepdims=True)
        scale = lax.rsqrt(squares + 1e-06)
        a = full * scale * scale
        eye = jnp.where(at_diag, 3.4445, 0.0)
        mix = None
        for step in range(ITERS):
            m = eye - 4.775 * a + 2.0315 * dot(a, a)
            if step < ITERS - 1:
                a = dot(dot(m, a), m)
            mix = m if mix is None else dot(m, mix)
        mix = mix * scale
        y = dot(mix, held[j].reshape(total_rows, cols))
        made[j] = y.reshape(nz, rows, cols)

        def far_one(k, c):
            give(j, far(k))
            return c

        def near_one(k, c):
            give(j, near(k))
            return c

        def inner_one(k, c):
            give(j, (1 - my_half) * half + my_half * quarter + k)
            return c

        lax.fori_loop(0, quarter, far_one, 0)
        lax.fori_loop(0, quarter, inner_one, 0)
        lax.fori_loop(1, half, near_one, 0)
        back[me, j] = made[j, me]

    gram_of(0)

    def stage(j, c):
        gram_of(j)
        finish(j - 1)
        return c

    lax.fori_loop(1, mine, stage, 0)
    finish(mine - 1)

    pltpu.make_async_copy(weights, res, weight_sem).wait()

    def update(j, c):
        came = back.at[pl.ds(0, nz - 1), j]
        pltpu.make_async_copy(came, came, ret_recv.at[j]).wait()

        def one(k, c):
            res[k, j] = (1.0 - learn_rate * decay_rate) * res[k, j] - learn_rate * back[k, j]
            return c

        return lax.fori_loop(0, nz, one, c)

    lax.fori_loop(0, mine, update, 0)

    others = sent.at[pl.ds(0, nz - 1)]
    pltpu.make_async_copy(others, others, fwd_send).wait()
    pltpu.make_async_copy(heard, heard, gram_send).wait()
    pltpu.make_async_copy(others, others, ret_send).wait()


def leave(res, mom, new_weights, new_momentum, sems):
    def copies(k):
        return (
            pltpu.make_async_copy(res.at[k], new_weights.at[k], sems.at[0, k]),
            pltpu.make_async_copy(mom.at[k], new_momentum.at[k], sems.at[1, k]),
        )

    def go(k, c):
        for copy in copies(k):
            copy.start()
        return c

    def end(k, c):
        for copy in copies(k):
            copy.wait()
        return c

    lax.fori_loop(0, res.shape[0], go, 0)
    lax.fori_loop(0, res.shape[0], end, 0)


def stepped(nz, nw, slopes, moments, weights):
    mats, rows, cols = slopes.shape
    mine = mats // nz
    n = nz * rows
    split = (nz, mine, rows, cols)
    hbm = pl.BlockSpec(memory_space=pltpu.HBM)
    buffer = pltpu.VMEM(split, jnp.float32)
    gathered = pltpu.VMEM((mine, nz, rows, cols), jnp.float32)
    each = pltpu.SemaphoreType.DMA((mine,))
    once = pltpu.SemaphoreType.DMA
    out, mom = pl.pallas_call(
        functools.partial(kernel, nz, nw),
        out_shape=(pltpu.VMEM(split, jnp.float32),) * 2,
        in_specs=[hbm] * 3,
        out_specs=[pl.BlockSpec(memory_space=pltpu.VMEM)] * 2,
        scratch_shapes=[
            buffer,
            gathered,
            gathered,
            buffer,
            pltpu.VMEM((mine, n, n), jnp.float32),
            pltpu.VMEM((mine, nw - 1, n, n), jnp.float32),
            pltpu.SemaphoreType.DMA((nz,)),
            pltpu.SemaphoreType.DMA((nz,)),
            once,
            once,
            each,
            each,
            once,
            each,
            once,
            each,
        ],
        compiler_params=pltpu.CompilerParams(
            collective_id=0, has_side_effects=True, vmem_limit_bytes=35 * 1024 * 1024
        ),
        name="stepped",
    )(slopes.reshape(split), moments.reshape(split), weights.reshape(split))
    out, mom = pl.pallas_call(
        leave,
        out_shape=(jax.ShapeDtypeStruct(split, jnp.float32),) * 2,
        in_specs=[pl.BlockSpec(memory_space=pltpu.VMEM)] * 2,
        out_specs=[hbm] * 2,
        scratch_shapes=[pltpu.SemaphoreType.DMA((2, nz))],
        compiler_params=pltpu.CompilerParams(vmem_limit_bytes=1024 * 1024),
        name="leave",
    )(out, mom)
    return out.reshape(slopes.shape), mom.reshape(slopes.shape)


def body(nz, nw, slopes_in, moments_in, weights_in):
    return stepped(nz, nw, slopes_in, moments_in, weights_in)


def solution(mesh):
    spec = P(None, "zero", "width")
    run = functools.partial(body, mesh.shape["zero"], mesh.shape["width"])
    return jax.shard_map(run, mesh=mesh, in_specs=(spec,) * 3, out_specs=(spec,) * 2, check_vma=False)
```

```python
import functools

import jax
import jax.numpy as jnp
from jax import lax
from jax.experimental import pallas as pl
from jax.experimental.pallas import tpu as pltpu
from jax.sharding import PartitionSpec as P

ITERS = 3
MESH = pl.DeviceIdType.MESH

hold_rate = 0.8
learn_rate = 0.8
decay_rate = 0.1


def dot(a, b):
    return jnp.dot(a, b, precision=lax.Precision.HIGHEST, preferred_element_type=jnp.float32)


def kernel(
    nz, nw, slopes, moments, weights, res, mom, sent, held, made, back, gram, heard,
    slope_sem, moment_sem, weight_sem, fwd_send, fwd_recv, own_sem, gram_send, gram_recv, ret_send, ret_recv,
):
    me = lax.axis_index("zero")
    side = lax.axis_index("width")
    _, mine, rows, cols = sent.shape
    total_rows = nz * rows
    half = nz // 2
    quarter = nz // 4
    my_half = me // half
    my_quarter = me // quarter
    inner = jnp.logical_and(my_quarter >= 1, my_quarter <= 2)
    partner = my_half * quarter + (1 - my_half) * half + lax.rem(me, quarter)

    def far(k):
        outer = 1 - k // quarter
        return (1 - my_half) * (half + outer * quarter) + my_half * (1 - outer) * quarter + lax.rem(me + k, quarter)

    def near(k):
        return my_half * half + lax.rem(me + k, half)

    barrier = pltpu.get_barrier_semaphore()

    def greet(to, across):
        pl.semaphore_signal(barrier, inc=1, device_id=(to, lax.rem(side + across, nw)), device_id_type=MESH)

    def inner_of(k):
        return quarter + lax.rem(me + quarter + k, half)

    def outer_of(k):
        return lax.rem(half + quarter + lax.rem(me + quarter + k, half), nz)

    @pl.when(inner)
    def _():
        greet(partner, 0)

    @pl.when(jnp.logical_not(inner))
    def _():
        def greet_outer(k, c):
            greet(outer_of(k), 0)
            return c

        def greet_across(k, c):
            greet(me, k)
            return c

        lax.fori_loop(1, half, greet_outer, 0)
        lax.fori_loop(1, nw, greet_across, 0)

    def slope_copy(k):
        return pltpu.make_async_copy(slopes.at[k], sent.at[k], slope_sem.at[k])

    def moment_copy(k):
        return pltpu.make_async_copy(moments.at[k], mom.at[k], moment_sem.at[k])

    def load(k):
        slope_copy(k).start()
        moment_copy(k).start()

    def direction(k):
        slope_copy(k).wait()
        moment_copy(k).wait()

        def one(j, c):
            slope = sent[k, j]
            fresh = hold_rate * mom[k, j] + slope
            mom[k, j] = fresh
            sent[k, j] = hold_rate * fresh + slope
            return c

        lax.fori_loop(0, mine, one, 0)

    def send(j, to):
        pltpu.make_async_remote_copy(
            src_ref=sent.at[to, j],
            dst_ref=held.at[j, me],
            send_sem=fwd_send,
            recv_sem=fwd_recv.at[j],
            device_id=(to, side),
            device_id_type=MESH,
        ).start()

    def other(k):
        return lax.rem(partner + k, nz)

    load(partner)

    def load_one(k, c):
        load(other(k))
        return c

    def direction_one(k, c):
        direction(other(k))
        return c

    lax.fori_loop(1, nz, load_one, 0)
    direction(partner)

    @pl.when(inner)
    def _():
        pl.semaphore_wait(barrier, 1)

        def early(j, c):
            send(j, partner)
            return c

        lax.fori_loop(0, mine, early, 0)

        def greet_outer(k, c):
            def one(across, c):
                greet(outer_of(k), across)
                return c

            return lax.fori_loop(0, nw, one, c)

        lax.fori_loop(0, half, greet_outer, 0)

    lax.fori_loop(1, nz, direction_one, 0)

    @pl.when(inner)
    def _():
        pl.semaphore_wait(barrier, half)

    @pl.when(jnp.logical_not(inner))
    def _():
        pl.semaphore_wait(barrier, half - 1 + nw - 1 + half * nw)

        def greet_inner(k, c):
            greet(inner_of(k), 0)
            return c

        lax.fori_loop(0, half, greet_inner, 0)

    def forward(j, c):
        def far_one(k, c):
            send(j, far(k))
            return c

        def near_one(k, c):
            send(j, near(k))
            return c

        lax.fori_loop(0, quarter, far_one, 0)

        @pl.when(inner)
        def _():
            lax.fori_loop(quarter + 1, half, far_one, 0)

        @pl.when(jnp.logical_not(inner))
        def _():
            lax.fori_loop(quarter, half, far_one, 0)

        lax.fori_loop(1, half, near_one, 0)
        pltpu.make_async_copy(sent.at[me, j], held.at[j, me], own_sem.at[j]).start()
        return c

    lax.fori_loop(0, mine, forward, 0)
    pltpu.make_async_copy(weights, res, weight_sem).start()

    def gram_of(j):
        others = held.at[j, pl.ds(0, nz - 1)]
        pltpu.make_async_copy(others, others, fwd_recv.at[j]).wait()
        pltpu.make_async_copy(sent.at[me, j], held.at[j, me], own_sem.at[j]).wait()
        x = held[j].reshape(total_rows, cols)
        gram[j] = lax.dot_general(
            x, x, (((1,), (1,)), ((), ())),
            precision=lax.Precision.HIGHEST, preferred_element_type=jnp.float32,
        )

        def one(k, c):
            to = lax.rem(side + k, nw)
            pltpu.make_async_remote_copy(
                src_ref=gram.at[j],
                dst_ref=heard.at[j, k - 1],
                send_sem=gram_send,
                recv_sem=gram_recv.at[j],
                device_id=(me, to),
                device_id_type=MESH,
            ).start()
            return c

        lax.fori_loop(1, nw, one, 0)

    def give(j, to):
        pltpu.make_async_remote_copy(
            src_ref=made.at[j, to],
            dst_ref=back.at[me, j],
            send_sem=ret_send,
            recv_sem=ret_recv.at[j],
            device_id=(to, side),
            device_id_type=MESH,
        ).start()

    def finish(j):
        pltpu.make_async_copy(heard.at[j], heard.at[j], gram_recv.at[j]).wait()
        full = gram[j] + jnp.sum(heard[j], axis=0)
        at_diag = lax.broadcasted_iota(jnp.int32, full.shape, 0) == lax.broadcasted_iota(jnp.int32, full.shape, 1)
        squares = jnp.sum(jnp.sum(jnp.where(at_diag, full, 0.0), axis=1, keepdims=True), axis=0, keepdims=True)
        scale = lax.rsqrt(squares + 1e-06)
        a = full * scale * scale
        eye = jnp.where(at_diag, 3.4445, 0.0)
        mix = None
        for step in range(ITERS):
            m = eye - 4.775 * a + 2.0315 * dot(a, a)
            if step < ITERS - 1:
                a = dot(dot(m, a), m)
            mix = m if mix is None else dot(m, mix)
        mix = mix * scale
        y = dot(mix, held[j].reshape(total_rows, cols))
        made[j] = y.reshape(nz, rows, cols)

        def far_one(k, c):
            give(j, far(k))
            return c

        def near_one(k, c):
            give(j, near(k))
            return c

        def inner_one(k, c):
            give(j, (1 - my_half) * half + my_half * quarter + k)
            return c

        def outer_one(k, c):
            give(j, (1 - my_half) * (half + quarter) + k)
            return c

        lax.fori_loop(0, quarter, outer_one, 0)
        lax.fori_loop(0, quarter, inner_one, 0)
        lax.fori_loop(1, half, near_one, 0)
        back[me, j] = made[j, me]

    gram_of(0)

    def stage(j, c):
        gram_of(j)
        finish(j - 1)
        return c

    lax.fori_loop(1, mine, stage, 0)
    finish(mine - 1)

    pltpu.make_async_copy(weights, res, weight_sem).wait()

    def update(j, c):
        came = back.at[pl.ds(0, nz - 1), j]
        pltpu.make_async_copy(came, came, ret_recv.at[j]).wait()

        def one(k, c):
            res[k, j] = (1.0 - learn_rate * decay_rate) * res[k, j] - learn_rate * back[k, j]
            return c

        return lax.fori_loop(0, nz, one, c, unroll=4)

    lax.fori_loop(0, mine, update, 0)

    others = sent.at[pl.ds(0, nz - 1)]
    pltpu.make_async_copy(others, others, fwd_send).wait()
    pltpu.make_async_copy(heard, heard, gram_send).wait()
    pltpu.make_async_copy(others, others, ret_send).wait()


def leave(res, mom, new_weights, new_momentum, sems):
    def copies(k):
        return (
            pltpu.make_async_copy(res.at[k], new_weights.at[k], sems.at[0, k]),
            pltpu.make_async_copy(mom.at[k], new_momentum.at[k], sems.at[1, k]),
        )

    def go(k, c):
        for copy in copies(k):
            copy.start()
        return c

    def end(k, c):
        for copy in copies(k):
            copy.wait()
        return c

    lax.fori_loop(0, res.shape[0], go, 0)
    lax.fori_loop(0, res.shape[0], end, 0)


def stepped(nz, nw, slopes, moments, weights):
    mats, rows, cols = slopes.shape
    mine = mats // nz
    n = nz * rows
    split = (nz, mine, rows, cols)
    hbm = pl.BlockSpec(memory_space=pltpu.HBM)
    buffer = pltpu.VMEM(split, jnp.float32)
    gathered = pltpu.VMEM((mine, nz, rows, cols), jnp.float32)
    each = pltpu.SemaphoreType.DMA((mine,))
    once = pltpu.SemaphoreType.DMA
    out, mom = pl.pallas_call(
        functools.partial(kernel, nz, nw),
        out_shape=(pltpu.VMEM(split, jnp.float32),) * 2,
        in_specs=[hbm] * 3,
        out_specs=[pl.BlockSpec(memory_space=pltpu.VMEM)] * 2,
        scratch_shapes=[
            buffer,
            gathered,
            gathered,
            buffer,
            pltpu.VMEM((mine, n, n), jnp.float32),
            pltpu.VMEM((mine, nw - 1, n, n), jnp.float32),
            pltpu.SemaphoreType.DMA((nz,)),
            pltpu.SemaphoreType.DMA((nz,)),
            once,
            once,
            each,
            each,
            once,
            each,
            once,
            each,
        ],
        compiler_params=pltpu.CompilerParams(
            collective_id=0, has_side_effects=True, vmem_limit_bytes=35 * 1024 * 1024
        ),
        name="stepped",
    )(slopes.reshape(split), moments.reshape(split), weights.reshape(split))
    out, mom = pl.pallas_call(
        leave,
        out_shape=(jax.ShapeDtypeStruct(split, jnp.float32),) * 2,
        in_specs=[pl.BlockSpec(memory_space=pltpu.VMEM)] * 2,
        out_specs=[hbm] * 2,
        scratch_shapes=[pltpu.SemaphoreType.DMA((2, nz))],
        compiler_params=pltpu.CompilerParams(vmem_limit_bytes=1024 * 1024),
        name="leave",
    )(out, mom)
    return out.reshape(slopes.shape), mom.reshape(slopes.shape)


def body(nz, nw, slopes_in, moments_in, weights_in):
    return stepped(nz, nw, slopes_in, moments_in, weights_in)


def solution(mesh):
    spec = P(None, "zero", "width")
    run = functools.partial(body, mesh.shape["zero"], mesh.shape["width"])
    return jax.shard_map(run, mesh=mesh, in_specs=(spec,) * 3, out_specs=(spec,) * 2, check_vma=False)
```

```python
import functools

import jax
import jax.numpy as jnp
from jax import lax
from jax.experimental import pallas as pl
from jax.experimental.pallas import tpu as pltpu
from jax.sharding import PartitionSpec as P

ITERS = 3
MESH = pl.DeviceIdType.MESH

hold_rate = 0.8
learn_rate = 0.8
decay_rate = 0.1


def dot(a, b):
    return jnp.dot(a, b, precision=lax.Precision.HIGHEST, preferred_element_type=jnp.float32)


def kernel(
    nz, nw, slopes, moments, weights, res, mom, sent, held, made, back, gram, heard,
    slope_sem, moment_sem, weight_sem, fwd_send, fwd_recv, own_sem, gram_send, gram_recv, ret_send, ret_recv,
):
    me = lax.axis_index("zero")
    side = lax.axis_index("width")
    _, mine, rows, cols = sent.shape
    total_rows = nz * rows
    half = nz // 2
    quarter = nz // 4
    my_half = me // half
    my_quarter = me // quarter
    inner = jnp.logical_and(my_quarter >= 1, my_quarter <= 2)
    partner = my_half * quarter + (1 - my_half) * half + lax.rem(me, quarter)

    def far(k):
        outer = 1 - k // quarter
        return (1 - my_half) * (half + outer * quarter) + my_half * (1 - outer) * quarter + lax.rem(me + k, quarter)

    def near(k):
        return my_half * half + lax.rem(me + k, half)

    barrier = pltpu.get_barrier_semaphore()

    def greet(to, across):
        pl.semaphore_signal(barrier, inc=1, device_id=(to, lax.rem(side + across, nw)), device_id_type=MESH)

    def inner_of(k):
        return quarter + lax.rem(me + quarter + k, half)

    def outer_of(k):
        return lax.rem(half + quarter + lax.rem(me + quarter + k, half), nz)

    @pl.when(inner)
    def _():
        greet(partner, 0)

    @pl.when(jnp.logical_not(inner))
    def _():
        def greet_outer(k, c):
            greet(outer_of(k), 0)
            return c

        def greet_across(k, c):
            greet(me, k)
            return c

        lax.fori_loop(1, half, greet_outer, 0)
        lax.fori_loop(1, nw, greet_across, 0)

    def slope_copy(k):
        return pltpu.make_async_copy(slopes.at[k], sent.at[k], slope_sem.at[k])

    def moment_copy(k):
        return pltpu.make_async_copy(moments.at[k], mom.at[k], moment_sem.at[k])

    def load(k):
        slope_copy(k).start()
        moment_copy(k).start()

    def direction(k):
        slope_copy(k).wait()
        moment_copy(k).wait()

        def one(j, c):
            slope = sent[k, j]
            fresh = hold_rate * mom[k, j] + slope
            mom[k, j] = fresh
            sent[k, j] = hold_rate * fresh + slope
            return c

        lax.fori_loop(0, mine, one, 0)

    def send(j, to):
        pltpu.make_async_remote_copy(
            src_ref=sent.at[to, j],
            dst_ref=held.at[j, me],
            send_sem=fwd_send,
            recv_sem=fwd_recv.at[j],
            device_id=(to, side),
            device_id_type=MESH,
        ).start()

    def other(k):
        return lax.rem(partner + k, nz)

    load(partner)

    def load_one(k, c):
        load(other(k))
        return c

    def direction_one(k, c):
        direction(other(k))
        return c

    lax.fori_loop(1, nz, load_one, 0)
    direction(partner)

    @pl.when(inner)
    def _():
        pl.semaphore_wait(barrier, 1)

        def early(j, c):
            send(j, partner)
            return c

        lax.fori_loop(0, mine, early, 0)

        def greet_outer(k, c):
            def one(across, c):
                greet(outer_of(k), across)
                return c

            return lax.fori_loop(0, nw, one, c)

        lax.fori_loop(0, half, greet_outer, 0)

    lax.fori_loop(1, nz, direction_one, 0)

    @pl.when(inner)
    def _():
        pl.semaphore_wait(barrier, half)

    @pl.when(jnp.logical_not(inner))
    def _():
        pl.semaphore_wait(barrier, half - 1 + nw - 1 + half * nw)

        def greet_inner(k, c):
            greet(inner_of(k), 0)
            return c

        lax.fori_loop(0, half, greet_inner, 0)

    def forward(j, c):
        def far_one(k, c):
            send(j, far(k))
            return c

        def near_one(k, c):
            send(j, near(k))
            return c

        lax.fori_loop(0, quarter, far_one, 0)

        @pl.when(inner)
        def _():
            lax.fori_loop(quarter + 1, half, far_one, 0)

        @pl.when(jnp.logical_not(inner))
        def _():
            lax.fori_loop(quarter, half, far_one, 0)

        lax.fori_loop(1, half, near_one, 0)
        pltpu.make_async_copy(sent.at[me, j], held.at[j, me], own_sem.at[j]).start()
        return c

    lax.fori_loop(0, mine, forward, 0)
    pltpu.make_async_copy(weights, res, weight_sem).start()

    def gram_of(j):
        others = held.at[j, pl.ds(0, nz - 1)]
        pltpu.make_async_copy(others, others, fwd_recv.at[j]).wait()
        pltpu.make_async_copy(sent.at[me, j], held.at[j, me], own_sem.at[j]).wait()
        x = held[j].reshape(total_rows, cols)
        gram[j] = lax.dot_general(
            x, x, (((1,), (1,)), ((), ())),
            precision=lax.Precision.HIGHEST, preferred_element_type=jnp.float32,
        )

        def one(k, c):
            to = lax.rem(side + k, nw)
            pltpu.make_async_remote_copy(
                src_ref=gram.at[j],
                dst_ref=heard.at[j, k - 1],
                send_sem=gram_send,
                recv_sem=gram_recv.at[j],
                device_id=(me, to),
                device_id_type=MESH,
            ).start()
            return c

        lax.fori_loop(1, nw, one, 0)

    def give(j, to):
        pltpu.make_async_remote_copy(
            src_ref=made.at[j, to],
            dst_ref=back.at[me, j],
            send_sem=ret_send,
            recv_sem=ret_recv.at[j],
            device_id=(to, side),
            device_id_type=MESH,
        ).start()

    def finish(j):
        pltpu.make_async_copy(heard.at[j], heard.at[j], gram_recv.at[j]).wait()
        full = gram[j] + jnp.sum(heard[j], axis=0)
        at_diag = lax.broadcasted_iota(jnp.int32, full.shape, 0) == lax.broadcasted_iota(jnp.int32, full.shape, 1)
        squares = jnp.sum(jnp.sum(jnp.where(at_diag, full, 0.0), axis=1, keepdims=True), axis=0, keepdims=True)
        scale = lax.rsqrt(squares + 1e-06)
        a = full * scale * scale
        eye = jnp.where(at_diag, 3.4445, 0.0)
        mix = None
        for step in range(ITERS):
            m = eye - 4.775 * a + 2.0315 * dot(a, a)
            if step < ITERS - 1:
                a = dot(dot(m, a), m)
            mix = m if mix is None else dot(m, mix)
        mix = mix * scale
        y = dot(mix, held[j].reshape(total_rows, cols))
        made[j] = y.reshape(nz, rows, cols)

        def far_one(k, c):
            give(j, far(k))
            return c

        def near_one(k, c):
            give(j, near(k))
            return c

        def inner_one(k, c):
            give(j, (1 - my_half) * half + my_half * quarter + k)
            return c

        def outer_one(k, c):
            give(j, (1 - my_half) * (half + quarter) + k)
            return c

        lax.fori_loop(0, quarter, outer_one, 0)
        lax.fori_loop(0, quarter, inner_one, 0)
        lax.fori_loop(1, half, near_one, 0)
        back[me, j] = made[j, me]

    gram_of(0)

    def stage(j, c):
        gram_of(j)
        finish(j - 1)
        return c

    lax.fori_loop(1, mine, stage, 0)
    finish(mine - 1)

    pltpu.make_async_copy(weights, res, weight_sem).wait()

    others = sent.at[pl.ds(0, nz - 1)]
    pltpu.make_async_copy(others, others, fwd_send).wait()
    pltpu.make_async_copy(heard, heard, gram_send).wait()

    def update(j, c):
        came = back.at[pl.ds(0, nz - 1), j]
        pltpu.make_async_copy(came, came, ret_recv.at[j]).wait()

        def one(k, c):
            res[k, j] = (1.0 - learn_rate * decay_rate) * res[k, j] - learn_rate * back[k, j]
            return c

        return lax.fori_loop(0, nz, one, c, unroll=8)

    lax.fori_loop(0, mine, update, 0)

    pltpu.make_async_copy(others, others, ret_send).wait()


def leave(res, mom, new_weights, new_momentum, sems):
    def copies(k):
        return (
            pltpu.make_async_copy(res.at[k], new_weights.at[k], sems.at[0, k]),
            pltpu.make_async_copy(mom.at[k], new_momentum.at[k], sems.at[1, k]),
        )

    def go(k, c):
        for copy in copies(k):
            copy.start()
        return c

    def end(k, c):
        for copy in copies(k):
            copy.wait()
        return c

    lax.fori_loop(0, res.shape[0], go, 0)
    lax.fori_loop(0, res.shape[0], end, 0)


def stepped(nz, nw, slopes, moments, weights):
    mats, rows, cols = slopes.shape
    mine = mats // nz
    n = nz * rows
    split = (nz, mine, rows, cols)
    hbm = pl.BlockSpec(memory_space=pltpu.HBM)
    buffer = pltpu.VMEM(split, jnp.float32)
    gathered = pltpu.VMEM((mine, nz, rows, cols), jnp.float32)
    each = pltpu.SemaphoreType.DMA((mine,))
    once = pltpu.SemaphoreType.DMA
    out, mom = pl.pallas_call(
        functools.partial(kernel, nz, nw),
        out_shape=(pltpu.VMEM(split, jnp.float32),) * 2,
        in_specs=[hbm] * 3,
        out_specs=[pl.BlockSpec(memory_space=pltpu.VMEM)] * 2,
        scratch_shapes=[
            buffer,
            gathered,
            gathered,
            buffer,
            pltpu.VMEM((mine, n, n), jnp.float32),
            pltpu.VMEM((mine, nw - 1, n, n), jnp.float32),
            pltpu.SemaphoreType.DMA((nz,)),
            pltpu.SemaphoreType.DMA((nz,)),
            once,
            once,
            each,
            each,
            once,
            each,
            once,
            each,
        ],
        compiler_params=pltpu.CompilerParams(
            collective_id=0, has_side_effects=True, vmem_limit_bytes=35 * 1024 * 1024
        ),
        name="stepped",
    )(slopes.reshape(split), moments.reshape(split), weights.reshape(split))
    out, mom = pl.pallas_call(
        leave,
        out_shape=(jax.ShapeDtypeStruct(split, jnp.float32),) * 2,
        in_specs=[pl.BlockSpec(memory_space=pltpu.VMEM)] * 2,
        out_specs=[hbm] * 2,
        scratch_shapes=[pltpu.SemaphoreType.DMA((2, nz))],
        compiler_params=pltpu.CompilerParams(vmem_limit_bytes=1024 * 1024),
        name="leave",
    )(out, mom)
    return out.reshape(slopes.shape), mom.reshape(slopes.shape)


def body(nz, nw, slopes_in, moments_in, weights_in):
    return stepped(nz, nw, slopes_in, moments_in, weights_in)


def solution(mesh):
    spec = P(None, "zero", "width")
    run = functools.partial(body, mesh.shape["zero"], mesh.shape["width"])
    return jax.shard_map(run, mesh=mesh, in_specs=(spec,) * 3, out_specs=(spec,) * 2, check_vma=False)
```
